32 devices in a mesh: blk: 16 (over z, y, x), rep: 2 (over core).
Axes of the slice: x: 2, y: 2, z: 4, core: 2. Of those that a mesh axis runs over, the one named last changes fastest.
Arguments:
- load_coef: bfloat16 [32, 2049, 256], P('blk', None, 'rep'), parts along dimension 2, may hold values from -0.29882812 to 0.29882812
- legendre: bfloat16 [32, 2049, 1024], P('blk'), may hold values from -0.125 to 0.125
- slab_orders: int32 [32], replicated, may hold values from 0 to 1023, as said below
- cycle_rows: int32 [1024], replicated, may hold values from 0 to 1023, each once
Outputs:
- potential: bfloat16 [1024, 128, 4096], P('blk', 'rep'), parts along dimension 1
- energy: float32 [128], P('rep'), parts along dimension 0
The draws below stay inside these ranges and needn't reach their ends.
There are 2 independent parts, one for each index of `rep`. The reference program is written for one: setup_inputs(seed, part) draws one part's arguments, and reference() takes and returns one part's arrays. A program takes and returns all parts, laid end to end along the dimension named above; an argument that names none is the same for every part. Nothing has to cross between parts.
Inputs may be any that keep to these rules, and one draw needn't show every extreme that they name: `slab_orders`: values are distinct and below (2048) / 2. `cycle_rows`: each cycle appears once.
All inputs are finite; a program needn't handle non-finite values.
Results may differ from the reference program's by a relative error of at most 0.0055.
Values may be sent and summed in bfloat16 or wider, within the bound.
A program may use at most 192 MiB of HBM per device.

```python
import math
import jax
import jax.numpy as jnp
from jax import lax

DEGREE = 2047
NLAT = 1024
NLON = 4096
FIELDS = 64
SLAB = 2049
PAIRS = 32


def draw_slab_orders(key, part):
    return jax.random.permutation(key, (DEGREE + 1) // 2)[:PAIRS].astype(jnp.int32)


def levels(key, dims, shards, smallest, top_value):
    loudness = 1.0
    for axis_at, blocks in shards:
        draws = jax.random.uniform(jax.random.fold_in(jax.random.fold_in(key, 6), axis_at), (blocks,), jnp.float32, smallest / len(shards), top_value / len(shards))
        loudness = loudness * jnp.repeat(jnp.exp(draws), dims[axis_at] // blocks).reshape((-1,) + (1,) * (len(dims) - 1 - axis_at))
    return loudness


def scatter_about(key, dims, scale, limit, pieces=(), kind=jnp.bfloat16):
    values = jax.random.normal(key, dims, jnp.float32) * scale
    if len(pieces) > 0:
        values = levels(key, dims, pieces, -0.22, 0.18) * values
    return jnp.clip(values, min=-limit, max=limit).astype(kind)


def setup_inputs(seed: int = 0, part: int = 0) -> dict:
    streams_of = jax.random.split(jax.random.key(seed), 5)
    part_splits = jax.random.split(jax.random.fold_in(streams_of[4], part), 5)
    load_coef = scatter_about(part_splits[0], (PAIRS, SLAB, 2 * FIELDS), 0.05, 0.29882812, ((0, 16),))
    legendre = scatter_about(streams_of[1], (PAIRS, SLAB, NLAT), SLAB ** -0.5, 0.125, ((0, 16),))
    slab_orders = draw_slab_orders(jax.random.fold_in(streams_of[4], 71), part)
    cycle_rows = jax.random.permutation(streams_of[3], NLAT).astype(jnp.int32)
    return {"load_coef": load_coef, "legendre": legendre, "slab_orders": slab_orders, "cycle_rows": cycle_rows}


def basis_table(orders):
    longitude_ids = jnp.arange(NLON, dtype=jnp.int32)
    phase_ids = (orders[:, None] * longitude_ids[None, :]) % NLON
    angles = phase_ids.astype(jnp.float32) * (2.0 * math.pi / NLON)
    factor = jnp.where(orders == 0, 1.0, 2.0).astype(jnp.float32)[:, None]
    return (factor * jnp.cos(angles)).astype(jnp.bfloat16), (-factor * jnp.sin(angles)).astype(jnp.bfloat16)


def reference(load_coef, legendre, slab_orders, cycle_rows):
    slab_rows = DEGREE + 2
    row_ids = jnp.arange(slab_rows, dtype=jnp.int32)

    def synthesize(pair_args):
        pair_coef, pair_table, low_order = pair_args
        in_lower = (row_ids < slab_rows - 1 - low_order)[:, None]
        nothing = jnp.zeros_like(pair_coef)
        stacked = jnp.concatenate([jnp.where(in_lower, pair_coef, nothing), jnp.where(in_lower, nothing, pair_coef)], axis=1)
        return lax.dot_general(stacked, pair_table, (((0,), (0,)), ((), ())), preferred_element_type=jnp.float32).astype(jnp.bfloat16)

    spectra = lax.map(synthesize, (load_coef, legendre, slab_orders))
    spectra = spectra.reshape(PAIRS, 4, FIELDS, NLAT)
    cos_lower, sin_lower = basis_table(slab_orders.astype(jnp.int32))
    cos_upper, sin_upper = basis_table((DEGREE - slab_orders).astype(jnp.int32))
    basis = jnp.stack([cos_lower, sin_lower, cos_upper, sin_upper], axis=1).reshape(PAIRS * 4, NLON)

    def per_field(field_index):
        rows = spectra[:, :, field_index, :].reshape(PAIRS * 4, NLAT)
        wave = lax.dot_general(rows, basis, (((0,), (0,)), ((), ())), preferred_element_type=jnp.float32)
        energy = jnp.sum(wave * wave) / (NLAT * NLON)
        return wave[cycle_rows].astype(jnp.bfloat16), energy

    potential, energy = lax.map(per_field, jnp.arange(FIELDS, dtype=jnp.int32))
    return jnp.transpose(potential, (1, 0, 2)), energy
```

```python
import functools
import math

import jax
import jax.numpy as jnp
from jax import lax
from jax.experimental import pallas as pl
from jax.experimental.pallas import tpu as pltpu
from jax.sharding import PartitionSpec as P

NLON = 4096
LANES = 128
MESH = pl.DeviceIdType.MESH


def spectra_kernel(pairs, orders_ref, table_ref, coef_ref, rows_ref, send_ref, energy_ref, masked, spectra, staging):
    step = pl.program_id(0)
    packed_rows, block = table_ref.shape
    slab_rows = packed_rows // pairs
    streams = masked.shape[0] // (2 * pairs)

    @pl.when(step == 0)
    def _():
        flipped = jnp.transpose(coef_ref[...].astype(jnp.float32))
        packed_id = lax.broadcasted_iota(jnp.int32, flipped.shape, 1)
        row_id = packed_id // pairs
        pair_id = packed_id % pairs
        for pair in range(pairs):
            lower = row_id < slab_rows - 1 - orders_ref[pair]
            mine = pair_id == pair
            for half in range(2):
                keep = mine & (lower if half == 0 else ~lower)
                start = (2 * pair + half) * streams
                masked[start : start + streams, :] = jnp.where(keep, flipped, 0.0).astype(jnp.bfloat16)

    product = jnp.dot(masked[:, :packed_rows], table_ref[...], preferred_element_type=jnp.float32)
    spectra[:, pl.ds(pl.multiple_of(step * block, block), block)] = product.astype(jnp.bfloat16)

    @pl.when(step == pl.num_programs(0) - 1)
    def _():
        lat_count = spectra.shape[1]
        fields = streams // 2
        groups = lat_count // 2
        kinds = 4 * pairs
        chunk = min(256, groups)
        total = jnp.zeros((1, kinds * fields), jnp.float32)
        for start in range(0, groups, chunk):
            sorted_rows = []
            for parity in range(2):
                wanted = rows_ref[parity * groups + start : parity * groups + start + chunk, :]
                cycle_id = lax.broadcasted_iota(jnp.int32, (chunk, lat_count), 1)
                chosen = (wanted == cycle_id).astype(jnp.float32).astype(jnp.bfloat16)
                rows = lax.dot_general(chosen, spectra[...], (((1,), (1,)), ((), ())), preferred_element_type=jnp.float32)
                total = total + jnp.sum(rows * rows, axis=0, keepdims=True)
                sorted_rows.append(rows)
            for kind in range(kinds):
                lanes = slice(kind * fields, (kind + 1) * fields)
                staging[pl.ds(start * kinds + kind, chunk, stride=kinds), :] = jnp.concatenate([sorted_rows[0][:, lanes], sorted_rows[1][:, lanes]], axis=1)
        energy = jnp.zeros((1, streams), jnp.float32)
        lane_id = lax.broadcasted_iota(jnp.int32, (1, streams), 1)
        for index in range(2 * pairs):
            part = total[:, index * streams : (index + 1) * streams]
            if index % 2 == 0:
                constant = orders_ref[index // 2] == 0
                weight = jnp.where(constant, jnp.where(lane_id < fields, 1.0, 0.0), 2.0)
            else:
                weight = 2.0
            energy = energy + weight * part
        energy_ref[...] = jnp.broadcast_to(energy, energy_ref.shape)
        send_ref[...] = staging[...].reshape(send_ref.shape).astype(jnp.bfloat16)


def exchange_kernel(n, degree, send_ref, energy_ref, orders_ref, recv_ref, basis_ref, total_ref, energies, send_sem, recv_sem, esend_sem, erecv_sem, own_sem):
    me = lax.axis_index("blk")
    barrier = pltpu.get_barrier_semaphore()

    def signal(s, carry):
        pl.semaphore_signal(barrier, inc=1, device_id={"blk": lax.rem(me + s, n)}, device_id_type=MESH)
        return carry

    lax.fori_loop(1, n, signal, 0)
    pl.semaphore_wait(barrier, n - 1)

    def block_copy(s):
        peer = lax.rem(me + s, n)
        return pltpu.make_async_remote_copy(
            src_ref=send_ref.at[peer], dst_ref=recv_ref.at[me], send_sem=send_sem.at[s], recv_sem=recv_sem.at[s],
            device_id={"blk": peer}, device_id_type=MESH)

    def energy_copy(s):
        peer = lax.rem(me + s, n)
        return pltpu.make_async_remote_copy(
            src_ref=energy_ref, dst_ref=energies.at[s], send_sem=esend_sem.at[s], recv_sem=erecv_sem.at[s],
            device_id={"blk": peer}, device_id_type=MESH)

    def start(s, carry):
        energy_copy(s).start()
        block_copy(s).start()
        return carry

    lax.fori_loop(1, n, start, 0)
    own = pltpu.make_async_copy(send_ref.at[me], recv_ref.at[me], own_sem)
    own.start()

    rows = basis_ref.shape[0]
    row_id = lax.broadcasted_iota(jnp.int32, (rows, LANES), 0)
    lane_id = lax.broadcasted_iota(jnp.int32, (rows, LANES), 1)
    low = jnp.broadcast_to(orders_ref[...], (rows, LANES))
    order = jnp.where((row_id & 2) == 0, low, degree - low)
    scale = 2.0 * math.pi / NLON
    turn = (order * (LANES * lane_id) + (row_id & 1) * (NLON // 4)) & (NLON - 1)
    fine = (order * lane_id) & (NLON - 1)
    factor = jnp.where(order == 0, 1.0, 2.0)
    coarse_angle = turn.astype(jnp.float32) * scale
    fine_angle = fine.astype(jnp.float32) * scale
    cos_coarse, sin_coarse = factor * jnp.cos(coarse_angle), factor * jnp.sin(coarse_angle)
    cos_fine, sin_fine = jnp.cos(fine_angle), jnp.sin(fine_angle)
    for tile in range(NLON // LANES):
        values = cos_coarse[:, tile : tile + 1] * cos_fine - sin_coarse[:, tile : tile + 1] * sin_fine
        basis_ref[:, tile * LANES : (tile + 1) * LANES] = values.astype(jnp.bfloat16)

    def finish_energy(s, total):
        energy_copy(s).wait()
        return total + energies[s]

    total_ref[...] = lax.fori_loop(1, n, finish_energy, energy_ref[...])

    def finish(s, carry):
        block_copy(s).wait()
        return carry

    lax.fori_loop(1, n, finish, 0)
    own.wait()


def wave_kernel(recv_ref, basis_ref, out_ref, held):
    groups = recv_ref.shape[1]
    depth = basis_ref.shape[0]
    for group in range(groups):
        values = recv_ref[:, group, :, :].astype(jnp.float32).reshape(depth, LANES)
        held[group * LANES : (group + 1) * LANES, :] = jnp.transpose(values).astype(jnp.bfloat16)
    width = 512

    @pl.loop(0, NLON // width)
    def _(tile):
        columns = pl.ds(pl.multiple_of(tile * width, width), width)
        wave = jnp.dot(held[...], basis_ref[:, columns], preferred_element_type=jnp.float32)
        out_ref[:, :, columns] = wave.astype(jnp.bfloat16).reshape(out_ref.shape[0], out_ref.shape[1], width)


def shards(load_coef, legendre, slab_orders, cycle_rows):
    n = lax.axis_size("blk")
    position = lax.axis_index("blk")
    pairs, slab_rows, streams = load_coef.shape
    fields = streams // 2
    lat_count = legendre.shape[2]
    cycle_count = lat_count // n
    per_tile = LANES // fields
    groups = cycle_count // per_tile
    kinds = 4 * pairs
    degree = slab_rows - 2
    packed_rows = slab_rows * pairs
    padded = -(-packed_rows // LANES) * LANES
    table = jnp.transpose(legendre, (1, 0, 2)).reshape(packed_rows, lat_count)
    coef = jnp.transpose(load_coef, (1, 0, 2)).reshape(packed_rows, streams)
    coef = jnp.pad(coef, ((0, padded - packed_rows), (0, 0)))
    my_orders = lax.dynamic_slice_in_dim(slab_orders, position * pairs, pairs)
    wanted = jnp.transpose(cycle_rows.reshape(lat_count // 2, 2)).reshape(lat_count, 1)
    steps = 4
    block = lat_count // steps
    send, energy = pl.pallas_call(
        functools.partial(spectra_kernel, pairs),
        grid_spec=pltpu.PrefetchScalarGridSpec(
            num_scalar_prefetch=1,
            grid=(steps,),
            in_specs=[
                pl.BlockSpec((packed_rows, block), lambda s, o: (0, s)),
                pl.BlockSpec((padded, streams), lambda s, o: (0, 0), pipeline_mode=pl.Buffered(1)),
                pl.BlockSpec((lat_count, 1), lambda s, o: (0, 0), pipeline_mode=pl.Buffered(1)),
            ],
            out_specs=[
                pl.BlockSpec((n, groups, kinds, LANES), lambda s, o: (0, 0, 0, 0)),
                pl.BlockSpec((8, streams), lambda s, o: (0, 0)),
            ],
            scratch_shapes=[
                pltpu.VMEM((2 * pairs * streams, padded), jnp.bfloat16),
                pltpu.VMEM((2 * pairs * streams, lat_count), jnp.bfloat16),
                pltpu.VMEM((n * groups * kinds, LANES), jnp.float32),
            ],
        ),
        out_shape=[
            jax.ShapeDtypeStruct((n, groups, kinds, LANES), jnp.bfloat16),
            jax.ShapeDtypeStruct((8, streams), jnp.float32),
        ],
        compiler_params=pltpu.CompilerParams(dimension_semantics=("arbitrary",)),
    )(my_orders, table, coef, wanted)
    order_rows = jnp.repeat(slab_orders, 4).reshape(n * kinds, 1)
    recv, basis, total = pl.pallas_call(
        functools.partial(exchange_kernel, n, degree),
        out_shape=[
            jax.ShapeDtypeStruct((n, groups, kinds, LANES), jnp.bfloat16),
            jax.ShapeDtypeStruct((n * kinds, NLON), jnp.bfloat16),
            jax.ShapeDtypeStruct((8, streams), jnp.float32),
        ],
        in_specs=[
            pl.BlockSpec(memory_space=pl.ANY),
            pl.BlockSpec(memory_space=pltpu.VMEM),
            pl.BlockSpec(memory_space=pltpu.VMEM),
        ],
        out_specs=[
            pl.BlockSpec(memory_space=pl.ANY),
            pl.BlockSpec(memory_space=pltpu.VMEM),
            pl.BlockSpec(memory_space=pltpu.VMEM),
        ],
        scratch_shapes=[
            pltpu.VMEM((n, 8, streams), jnp.float32),
            pltpu.SemaphoreType.DMA((n,)),
            pltpu.SemaphoreType.DMA((n,)),
            pltpu.SemaphoreType.DMA((n,)),
            pltpu.SemaphoreType.DMA((n,)),
            pltpu.SemaphoreType.DMA,
        ],
        compiler_params=pltpu.CompilerParams(collective_id=0, has_side_effects=True),
    )(send, energy, order_rows)
    step_groups = min(4, groups)
    potential = pl.pallas_call(
        wave_kernel,
        grid=(groups // step_groups,),
        out_shape=jax.ShapeDtypeStruct((cycle_count, fields, NLON), jnp.bfloat16),
        in_specs=[
            pl.BlockSpec((n, step_groups, kinds, LANES), lambda s: (0, s, 0, 0)),
            pl.BlockSpec((n * kinds, NLON), lambda s: (0, 0), pipeline_mode=pl.Buffered(1)),
        ],
        out_specs=pl.BlockSpec((step_groups * per_tile, fields, NLON), lambda s: (s, 0, 0)),
        scratch_shapes=[pltpu.VMEM((step_groups * LANES, n * kinds), jnp.bfloat16)],
        compiler_params=pltpu.CompilerParams(dimension_semantics=("arbitrary",)),
    )(recv, basis)
    energy = (total[0, :fields] + total[0, fields:]) / lat_count
    return potential, energy


def solution(mesh):
    in_specs = (P("blk", None, "rep"), P("blk", None, None), P(), P())
    out_specs = (P("blk", "rep", None), P("rep"))
    return jax.shard_map(shards, mesh=mesh, in_specs=in_specs, out_specs=out_specs, check_vma=False)
```

```python
import functools
import math

import jax
import jax.numpy as jnp
from jax import lax
from jax.experimental import pallas as pl
from jax.experimental.pallas import tpu as pltpu
from jax.sharding import PartitionSpec as P

NLON = 4096
LANES = 128
MESH = pl.DeviceIdType.MESH


def spectra_kernel(pairs, orders_ref, table_ref, coef_ref, rows_ref, send_ref, energy_ref, masked, spectra, sorted_rows, staging):
    step = pl.program_id(0)
    first_pair = lax.axis_index("blk") * pairs
    slab_rows, _, block = table_ref.shape
    packed_rows = slab_rows * pairs
    streams = masked.shape[0] // (2 * pairs)

    @pl.when(step == 0)
    def _():
        packed = coef_ref[...].reshape(packed_rows, streams)
        flipped = jnp.transpose(jnp.concatenate([packed, jnp.zeros((masked.shape[1] - packed_rows, streams), packed.dtype)], axis=0).astype(jnp.float32))
        packed_id = lax.broadcasted_iota(jnp.int32, flipped.shape, 1)
        row_id = packed_id // pairs
        pair_id = packed_id % pairs
        for pair in range(pairs):
            lower = row_id < slab_rows - 1 - orders_ref[first_pair + pair]
            mine = pair_id == pair
            for half in range(2):
                keep = mine & (lower if half == 0 else ~lower)
                start = (2 * pair + half) * streams
                masked[start : start + streams, :] = jnp.where(keep, flipped, 0.0).astype(jnp.bfloat16)

    product = jnp.dot(masked[:, :packed_rows], table_ref[...].reshape(packed_rows, block), preferred_element_type=jnp.float32)
    spectra[:, pl.ds(pl.multiple_of(step * block, block), block)] = product.astype(jnp.bfloat16)

    @pl.when(step == pl.num_programs(0) - 1)
    def _():
        lat_count = spectra.shape[1]
        fields = streams // 2
        kinds = 4 * pairs
        columns = jnp.transpose(rows_ref[...].astype(jnp.float32))
        cycle_id = lax.broadcasted_iota(jnp.int32, (LANES, lat_count), 1).astype(jnp.float32)
        total = jnp.zeros((1, kinds * fields), jnp.float32)
        half = LANES // 2
        for part in range(lat_count // LANES):
            chosen = (columns[:, part : part + 1] == cycle_id).astype(jnp.float32).astype(jnp.bfloat16)
            rows = lax.dot_general(chosen, spectra[...], (((1,), (1,)), ((), ())), preferred_element_type=jnp.float32)
            total = total + jnp.sum(rows * rows, axis=0, keepdims=True)
            for order in range(2 * pairs):
                sorted_rows[part, order] = rows[:, order * streams : (order + 1) * streams]
                even = sorted_rows[part, order, pl.ds(0, half, stride=2), :]
                odd = sorted_rows[part, order, pl.ds(1, half, stride=2), :]
                real = jnp.concatenate([even[:, :fields], odd[:, :fields]], axis=1)
                imag = jnp.concatenate([even[:, fields:], odd[:, fields:]], axis=1)
                first = part * half * kinds + 2 * order
                staging[pl.ds(first, half, stride=kinds), :] = real
                staging[pl.ds(first + 1, half, stride=kinds), :] = imag
        energy = jnp.zeros((1, streams), jnp.float32)
        lane_id = lax.broadcasted_iota(jnp.int32, (1, streams), 1)
        for index in range(2 * pairs):
            part = total[:, index * streams : (index + 1) * streams]
            if index % 2 == 0:
                constant = orders_ref[first_pair + index // 2] == 0
                weight = jnp.where(constant, jnp.where(lane_id < fields, 1.0, 0.0), 2.0)
            else:
                weight = 2.0
            energy = energy + weight * part
        energy_ref[...] = jnp.broadcast_to(energy, energy_ref.shape)
        send_ref[...] = staging[...].reshape(send_ref.shape).astype(jnp.bfloat16)


def exchange_kernel(n, degree, send_ref, energy_ref, orders_ref, recv_ref, basis_ref, total_ref, energies, send_sem, recv_sem, esend_sem, erecv_sem, own_sem):
    me = lax.axis_index("blk")
    barrier = pltpu.get_barrier_semaphore()

    def signal(s, carry):
        pl.semaphore_signal(barrier, inc=1, device_id={"blk": lax.rem(me + s, n)}, device_id_type=MESH)
        return carry

    lax.fori_loop(1, n, signal, 0)
    pl.semaphore_wait(barrier, n - 1)

    def block_copy(s):
        peer = lax.rem(me + s, n)
        return pltpu.make_async_remote_copy(
            src_ref=send_ref.at[peer], dst_ref=recv_ref.at[me], send_sem=send_sem.at[s], recv_sem=recv_sem.at[s],
            device_id={"blk": peer}, device_id_type=MESH)

    def energy_copy(s):
        peer = lax.rem(me + s, n)
        return pltpu.make_async_remote_copy(
            src_ref=energy_ref, dst_ref=energies.at[s], send_sem=esend_sem.at[s], recv_sem=erecv_sem.at[s],
            device_id={"blk": peer}, device_id_type=MESH)

    def start(s, carry):
        energy_copy(s).start()
        block_copy(s).start()
        return carry

    lax.fori_loop(1, n, start, 0)
    own = pltpu.make_async_copy(send_ref.at[me], recv_ref.at[me], own_sem)
    own.start()

    rows = basis_ref.shape[0]
    row_id = lax.broadcasted_iota(jnp.int32, (rows, LANES), 0)
    lane_id = lax.broadcasted_iota(jnp.int32, (rows, LANES), 1)
    width = orders_ref.shape[1]
    pair_row = lax.broadcasted_iota(jnp.int32, (rows, width), 0) // 4
    pair_lane = lax.broadcasted_iota(jnp.int32, (rows, width), 1)
    spread = jnp.where(pair_row == pair_lane, orders_ref[...].astype(jnp.float32), 0.0)
    low = jnp.broadcast_to(jnp.sum(spread, axis=1, keepdims=True), (rows, LANES)).astype(jnp.int32)
    order = jnp.where((row_id & 2) == 0, low, degree - low)
    scale = 2.0 * math.pi / NLON
    turn = (order * (LANES * lane_id) + (row_id & 1) * (NLON // 4)) & (NLON - 1)
    fine = (order * lane_id) & (NLON - 1)
    factor = jnp.where(order == 0, 1.0, 2.0)
    coarse_angle = turn.astype(jnp.float32) * scale
    fine_angle = fine.astype(jnp.float32) * scale
    cos_coarse, sin_coarse = factor * jnp.cos(coarse_angle), factor * jnp.sin(coarse_angle)
    cos_fine, sin_fine = jnp.cos(fine_angle), jnp.sin(fine_angle)
    for tile in range(NLON // LANES):
        values = cos_coarse[:, tile : tile + 1] * cos_fine - sin_coarse[:, tile : tile + 1] * sin_fine
        basis_ref[:, tile * LANES : (tile + 1) * LANES] = values.astype(jnp.bfloat16)

    def finish_energy(s, total):
        energy_copy(s).wait()
        return total + energies[s]

    total_ref[...] = lax.fori_loop(1, n, finish_energy, energy_ref[...])

    def finish(s, carry):
        block_copy(s).wait()
        return carry

    lax.fori_loop(1, n, finish, 0)
    own.wait()


def wave_kernel(scale, recv_ref, basis_ref, total_ref, out_ref, energy_ref, held):
    groups = recv_ref.shape[1]
    depth = basis_ref.shape[0]
    fields = out_ref.shape[1]
    for group in range(groups):
        values = recv_ref[:, group, :, :].astype(jnp.float32).reshape(depth, LANES)
        held[group * LANES : (group + 1) * LANES, :] = jnp.transpose(values).astype(jnp.bfloat16)
    width = min(NLON, NLON * LANES // depth)

    @pl.loop(0, NLON // width)
    def _(tile):
        columns = pl.ds(pl.multiple_of(tile * width, width), width)
        for cycle in range(out_ref.shape[0]):
            rows = held[cycle * fields : (cycle + 1) * fields, :]
            wave = jnp.dot(rows, basis_ref[:, columns], preferred_element_type=jnp.float32)
            out_ref[cycle, :, columns] = wave.astype(jnp.bfloat16)

    energy_ref[...] = (total_ref[0:1, :fields] + total_ref[0:1, fields:]) * scale


def shards(load_coef, legendre, slab_orders, cycle_rows):
    n = lax.axis_size("blk")
    pairs, slab_rows, streams = load_coef.shape
    fields = streams // 2
    lat_count = legendre.shape[2]
    cycle_count = lat_count // n
    per_tile = LANES // fields
    groups = cycle_count // per_tile
    kinds = 4 * pairs
    degree = slab_rows - 2
    packed_rows = slab_rows * pairs
    padded = -(-packed_rows // LANES) * LANES
    table = jnp.transpose(legendre, (1, 0, 2))
    coef = jnp.transpose(load_coef, (1, 0, 2))
    steps = 4
    block = lat_count // steps
    send, energy = pl.pallas_call(
        functools.partial(spectra_kernel, pairs),
        grid_spec=pltpu.PrefetchScalarGridSpec(
            num_scalar_prefetch=1,
            grid=(steps,),
            in_specs=[
                pl.BlockSpec((slab_rows, pairs, block), lambda s, o: (0, 0, s)),
                pl.BlockSpec((slab_rows, pairs, streams), lambda s, o: (0, 0, 0), pipeline_mode=pl.Buffered(1)),
                pl.BlockSpec((lat_count // LANES, LANES), lambda s, o: (0, 0), pipeline_mode=pl.Buffered(1)),
            ],
            out_specs=[
                pl.BlockSpec((n, groups, kinds, LANES), lambda s, o: (0, 0, 0, 0)),
                pl.BlockSpec((8, streams), lambda s, o: (0, 0)),
            ],
            scratch_shapes=[
                pltpu.VMEM((2 * pairs * streams, padded), jnp.bfloat16),
                pltpu.VMEM((2 * pairs * streams, lat_count), jnp.bfloat16),
                pltpu.VMEM((lat_count // LANES, 2 * pairs, LANES, streams), jnp.float32),
                pltpu.VMEM((n * groups * kinds, LANES), jnp.float32),
            ],
        ),
        out_shape=[
            jax.ShapeDtypeStruct((n, groups, kinds, LANES), jnp.bfloat16),
            jax.ShapeDtypeStruct((8, streams), jnp.float32),
        ],
        compiler_params=pltpu.CompilerParams(dimension_semantics=("arbitrary",)),
    )(slab_orders, table, coef, cycle_rows.reshape(lat_count // LANES, LANES))
    recv, basis, total = pl.pallas_call(
        functools.partial(exchange_kernel, n, degree),
        out_shape=[
            jax.ShapeDtypeStruct((n, groups, kinds, LANES), jnp.bfloat16),
            jax.ShapeDtypeStruct((n * kinds, NLON), jnp.bfloat16),
            jax.ShapeDtypeStruct((8, streams), jnp.float32),
        ],
        in_specs=[
            pl.BlockSpec(memory_space=pl.ANY),
            pl.BlockSpec(memory_space=pltpu.VMEM),
            pl.BlockSpec(memory_space=pltpu.VMEM),
        ],
        out_specs=[
            pl.BlockSpec(memory_space=pl.ANY),
            pl.BlockSpec(memory_space=pltpu.VMEM),
            pl.BlockSpec(memory_space=pltpu.VMEM),
        ],
        scratch_shapes=[
            pltpu.VMEM((n, 8, streams), jnp.float32),
            pltpu.SemaphoreType.DMA((n,)),
            pltpu.SemaphoreType.DMA((n,)),
            pltpu.SemaphoreType.DMA((n,)),
            pltpu.SemaphoreType.DMA((n,)),
            pltpu.SemaphoreType.DMA,
        ],
        compiler_params=pltpu.CompilerParams(collective_id=0, has_side_effects=True),
    )(send, energy, slab_orders.reshape(1, n * pairs))
    step_groups = min(4, groups)
    potential, mean_square = pl.pallas_call(
        functools.partial(wave_kernel, 1.0 / lat_count),
        grid=(groups // step_groups,),
        out_shape=[
            jax.ShapeDtypeStruct((cycle_count, fields, NLON), jnp.bfloat16),
            jax.ShapeDtypeStruct((1, fields), jnp.float32),
        ],
        in_specs=[
            pl.BlockSpec((n, step_groups, kinds, LANES), lambda s: (0, s, 0, 0)),
            pl.BlockSpec((n * kinds, NLON), lambda s: (0, 0), pipeline_mode=pl.Buffered(1)),
            pl.BlockSpec((8, streams), lambda s: (0, 0), pipeline_mode=pl.Buffered(1)),
        ],
        out_specs=[
            pl.BlockSpec((step_groups * per_tile, fields, NLON), lambda s: (s, 0, 0)),
            pl.BlockSpec((1, fields), lambda s: (0, 0)),
        ],
        scratch_shapes=[pltpu.VMEM((step_groups * LANES, n * kinds), jnp.bfloat16)],
        compiler_params=pltpu.CompilerParams(dimension_semantics=("arbitrary",)),
    )(recv, basis, total)
    return potential, mean_square.reshape(fields)


def solution(mesh):
    in_specs = (P("blk", None, "rep"), P("blk", None, None), P(), P())
    out_specs = (P("blk", "rep", None), P("rep"))
    return jax.shard_map(shards, mesh=mesh, in_specs=in_specs, out_specs=out_specs, check_vma=False)
```

```python
import functools
import math

import jax
import jax.numpy as jnp
from jax import lax
from jax.experimental import pallas as pl
from jax.experimental.pallas import tpu as pltpu
from jax.sharding import PartitionSpec as P

NLON = 4096
LANES = 128
MESH = pl.DeviceIdType.MESH


def spectra_kernel(pairs, orders_ref, table_ref, coef_ref, rows_ref, send_ref, energy_ref, masked, spectra, sorted_rows, staging):
    step = pl.program_id(0)
    first_pair = lax.axis_index("blk") * pairs
    slab_rows, _, block = table_ref.shape
    packed_rows = slab_rows * pairs
    streams = masked.shape[0] // (2 * pairs)

    @pl.when(step == 0)
    def _():
        packed = coef_ref[...].reshape(packed_rows, streams)
        flipped = jnp.transpose(jnp.concatenate([packed, jnp.zeros((masked.shape[1] - packed_rows, streams), packed.dtype)], axis=0).astype(jnp.float32))
        packed_id = lax.broadcasted_iota(jnp.int32, flipped.shape, 1)
        row_id = packed_id // pairs
        pair_id = packed_id % pairs
        for pair in range(pairs):
            lower = row_id < slab_rows - 1 - orders_ref[first_pair + pair]
            mine = pair_id == pair
            for half in range(2):
                keep = mine & (lower if half == 0 else ~lower)
                start = (2 * pair + half) * streams
                masked[start : start + streams, :] = jnp.where(keep, flipped, 0.0).astype(jnp.bfloat16)

    product = jnp.dot(masked[:, :packed_rows], table_ref[...].reshape(packed_rows, block), preferred_element_type=jnp.float32)
    spectra[:, pl.ds(pl.multiple_of(step * block, block), block)] = product.astype(jnp.bfloat16)

    @pl.when(step == pl.num_programs(0) - 1)
    def _():
        lat_count = spectra.shape[1]
        fields = streams // 2
        kinds = 4 * pairs
        columns = jnp.transpose(rows_ref[...].astype(jnp.float32))
        cycle_id = lax.broadcasted_iota(jnp.int32, (LANES, lat_count), 1).astype(jnp.float32)
        total = jnp.zeros((1, kinds * fields), jnp.float32)
        half = LANES // 2
        batch = min(4, lat_count // LANES)
        for first_part in range(0, lat_count // LANES, batch):
            chosen = jnp.concatenate(
                [(columns[:, first_part + i : first_part + i + 1] == cycle_id).astype(jnp.float32).astype(jnp.bfloat16) for i in range(batch)],
                axis=0,
            )
            rows = lax.dot_general(chosen, spectra[...], (((1,), (1,)), ((), ())), preferred_element_type=jnp.float32)
            total = total + jnp.sum(rows * rows, axis=0, keepdims=True)
            for part in range(first_part, first_part + batch):
                offset = (part - first_part) * LANES
                for order in range(2 * pairs):
                    sorted_rows[part, order] = rows[offset : offset + LANES, order * streams : (order + 1) * streams]
                    even = sorted_rows[part, order, pl.ds(0, half, stride=2), :]
                    odd = sorted_rows[part, order, pl.ds(1, half, stride=2), :]
                    real = jnp.concatenate([even[:, :fields], odd[:, :fields]], axis=1)
                    imag = jnp.concatenate([even[:, fields:], odd[:, fields:]], axis=1)
                    first = part * half * kinds + 2 * order
                    staging[pl.ds(first, half, stride=kinds), :] = real
                    staging[pl.ds(first + 1, half, stride=kinds), :] = imag
        energy = jnp.zeros((1, streams), jnp.float32)
        lane_id = lax.broadcasted_iota(jnp.int32, (1, streams), 1)
        for index in range(2 * pairs):
            part = total[:, index * streams : (index + 1) * streams]
            if index % 2 == 0:
                constant = orders_ref[first_pair + index // 2] == 0
                weight = jnp.where(constant, jnp.where(lane_id < fields, 1.0, 0.0), 2.0)
            else:
                weight = 2.0
            energy = energy + weight * part
        energy_ref[...] = jnp.broadcast_to(energy, energy_ref.shape)
        send_ref[...] = staging[...].reshape(send_ref.shape).astype(jnp.bfloat16)


def exchange_kernel(n, degree, send_ref, energy_ref, orders_ref, recv_ref, basis_ref, total_ref, energies, send_sem, recv_sem, esend_sem, erecv_sem, own_sem):
    me = lax.axis_index("blk")
    barrier = pltpu.get_barrier_semaphore()

    def signal(s, carry):
        pl.semaphore_signal(barrier, inc=1, device_id={"blk": lax.rem(me + s, n)}, device_id_type=MESH)
        return carry

    lax.fori_loop(1, n, signal, 0)
    pl.semaphore_wait(barrier, n - 1)

    def block_copy(s):
        peer = lax.rem(me + s, n)
        return pltpu.make_async_remote_copy(
            src_ref=send_ref.at[peer], dst_ref=recv_ref.at[me], send_sem=send_sem.at[s], recv_sem=recv_sem.at[s],
            device_id={"blk": peer}, device_id_type=MESH)

    def energy_copy(s):
        peer = lax.rem(me + s, n)
        return pltpu.make_async_remote_copy(
            src_ref=energy_ref, dst_ref=energies.at[s], send_sem=esend_sem.at[s], recv_sem=erecv_sem.at[s],
            device_id={"blk": peer}, device_id_type=MESH)

    def start(s, carry):
        energy_copy(s).start()
        block_copy(s).start()
        return carry

    lax.fori_loop(1, n, start, 0)
    own = pltpu.make_async_copy(send_ref.at[me], recv_ref.at[me], own_sem)
    own.start()

    rows = basis_ref.shape[0]
    row_id = lax.broadcasted_iota(jnp.int32, (rows, LANES), 0)
    lane_id = lax.broadcasted_iota(jnp.int32, (rows, LANES), 1)
    width = orders_ref.shape[1]
    pair_row = lax.broadcasted_iota(jnp.int32, (rows, width), 0) // 4
    pair_lane = lax.broadcasted_iota(jnp.int32, (rows, width), 1)
    spread = jnp.where(pair_row == pair_lane, orders_ref[...].astype(jnp.float32), 0.0)
    low = jnp.broadcast_to(jnp.sum(spread, axis=1, keepdims=True), (rows, LANES)).astype(jnp.int32)
    order = jnp.where((row_id & 2) == 0, low, degree - low)
    scale = 2.0 * math.pi / NLON
    turn = (order * (LANES * lane_id) + (row_id & 1) * (NLON // 4)) & (NLON - 1)
    fine = (order * lane_id) & (NLON - 1)
    factor = jnp.where(order == 0, 1.0, 2.0)
    coarse_angle = turn.astype(jnp.float32) * scale
    fine_angle = fine.astype(jnp.float32) * scale
    cos_coarse, sin_coarse = factor * jnp.cos(coarse_angle), factor * jnp.sin(coarse_angle)
    cos_fine, sin_fine = jnp.cos(fine_angle), jnp.sin(fine_angle)
    for tile in range(NLON // LANES):
        values = cos_coarse[:, tile : tile + 1] * cos_fine - sin_coarse[:, tile : tile + 1] * sin_fine
        basis_ref[:, tile * LANES : (tile + 1) * LANES] = values.astype(jnp.bfloat16)

    def finish_energy(s, total):
        energy_copy(s).wait()
        return total + energies[s]

    total_ref[...] = lax.fori_loop(1, n, finish_energy, energy_ref[...])

    def finish(s, carry):
        block_copy(s).wait()
        return carry

    lax.fori_loop(1, n, finish, 0)
    own.wait()


def wave_kernel(scale, recv_ref, basis_ref, total_ref, out_ref, energy_ref, held):
    groups = recv_ref.shape[1]
    depth = basis_ref.shape[0]
    fields = out_ref.shape[1]
    for group in range(groups):
        values = recv_ref[:, group, :, :].astype(jnp.float32).reshape(depth, LANES)
        held[group * LANES : (group + 1) * LANES, :] = jnp.transpose(values).astype(jnp.bfloat16)
    width = min(NLON, NLON * LANES // depth)

    @pl.loop(0, NLON // width)
    def _(tile):
        columns = pl.ds(pl.multiple_of(tile * width, width), width)
        for cycle in range(out_ref.shape[0]):
            rows = held[cycle * fields : (cycle + 1) * fields, :]
            wave = jnp.dot(rows, basis_ref[:, columns], preferred_element_type=jnp.float32)
            out_ref[cycle, :, columns] = wave.astype(jnp.bfloat16)

    energy_ref[...] = (total_ref[0:1, :fields] + total_ref[0:1, fields:]) * scale


def shards(load_coef, legendre, slab_orders, cycle_rows):
    n = lax.axis_size("blk")
    pairs, slab_rows, streams = load_coef.shape
    fields = streams // 2
    lat_count = legendre.shape[2]
    cycle_count = lat_count // n
    per_tile = LANES // fields
    groups = cycle_count // per_tile
    kinds = 4 * pairs
    degree = slab_rows - 2
    packed_rows = slab_rows * pairs
    padded = -(-packed_rows // LANES) * LANES
    table = jnp.transpose(legendre, (1, 0, 2))
    coef = jnp.transpose(load_coef, (1, 0, 2))
    steps = 4
    block = lat_count // steps
    send, energy = pl.pallas_call(
        functools.partial(spectra_kernel, pairs),
        grid_spec=pltpu.PrefetchScalarGridSpec(
            num_scalar_prefetch=1,
            grid=(steps,),
            in_specs=[
                pl.BlockSpec((slab_rows, pairs, block), lambda s, o: (0, 0, s)),
                pl.BlockSpec((slab_rows, pairs, streams), lambda s, o: (0, 0, 0), pipeline_mode=pl.Buffered(1)),
                pl.BlockSpec((lat_count // LANES, LANES), lambda s, o: (0, 0), pipeline_mode=pl.Buffered(1)),
            ],
            out_specs=[
                pl.BlockSpec((n, groups, kinds, LANES), lambda s, o: (0, 0, 0, 0)),
                pl.BlockSpec((8, streams), lambda s, o: (0, 0)),
            ],
            scratch_shapes=[
                pltpu.VMEM((2 * pairs * streams, padded), jnp.bfloat16),
                pltpu.VMEM((2 * pairs * streams, lat_count), jnp.bfloat16),
                pltpu.VMEM((lat_count // LANES, 2 * pairs, LANES, streams), jnp.float32),
                pltpu.VMEM((n * groups * kinds, LANES), jnp.float32),
            ],
        ),
        out_shape=[
            jax.ShapeDtypeStruct((n, groups, kinds, LANES), jnp.bfloat16),
            jax.ShapeDtypeStruct((8, streams), jnp.float32),
        ],
        compiler_params=pltpu.CompilerParams(dimension_semantics=("arbitrary",)),
    )(slab_orders, table, coef, cycle_rows.reshape(lat_count // LANES, LANES))
    recv, basis, total = pl.pallas_call(
        functools.partial(exchange_kernel, n, degree),
        out_shape=[
            jax.ShapeDtypeStruct((n, groups, kinds, LANES), jnp.bfloat16),
            jax.ShapeDtypeStruct((n * kinds, NLON), jnp.bfloat16),
            jax.ShapeDtypeStruct((8, streams), jnp.float32),
        ],
        in_specs=[
            pl.BlockSpec(memory_space=pl.ANY),
            pl.BlockSpec(memory_space=pltpu.VMEM),
            pl.BlockSpec(memory_space=pltpu.VMEM),
        ],
        out_specs=[
            pl.BlockSpec(memory_space=pl.ANY),
            pl.BlockSpec(memory_space=pltpu.VMEM),
            pl.BlockSpec(memory_space=pltpu.VMEM),
        ],
        scratch_shapes=[
            pltpu.VMEM((n, 8, streams), jnp.float32),
            pltpu.SemaphoreType.DMA((n,)),
            pltpu.SemaphoreType.DMA((n,)),
            pltpu.SemaphoreType.DMA((n,)),
            pltpu.SemaphoreType.DMA((n,)),
            pltpu.SemaphoreType.DMA,
        ],
        compiler_params=pltpu.CompilerParams(collective_id=0, has_side_effects=True),
    )(send, energy, slab_orders.reshape(1, n * pairs))
    step_groups = min(4, groups)
    potential, mean_square = pl.pallas_call(
        functools.partial(wave_kernel, 1.0 / lat_count),
        grid=(groups // step_groups,),
        out_shape=[
            jax.ShapeDtypeStruct((cycle_count, fields, NLON), jnp.bfloat16),
            jax.ShapeDtypeStruct((1, fields), jnp.float32),
        ],
        in_specs=[
            pl.BlockSpec((n, step_groups, kinds, LANES), lambda s: (0, s, 0, 0)),
            pl.BlockSpec((n * kinds, NLON), lambda s: (0, 0), pipeline_mode=pl.Buffered(1)),
            pl.BlockSpec((8, streams), lambda s: (0, 0), pipeline_mode=pl.Buffered(1)),
        ],
        out_specs=[
            pl.BlockSpec((step_groups * per_tile, fields, NLON), lambda s: (s, 0, 0)),
            pl.BlockSpec((1, fields), lambda s: (0, 0)),
        ],
        scratch_shapes=[pltpu.VMEM((step_groups * LANES, n * kinds), jnp.bfloat16)],
        compiler_params=pltpu.CompilerParams(dimension_semantics=("arbitrary",)),
    )(recv, basis, total)
    return potential, mean_square.reshape(fields)


def solution(mesh):
    in_specs = (P("blk", None, "rep"), P("blk", None, None), P(), P())
    out_specs = (P("blk", "rep", None), P("rep"))
    return jax.shard_map(shards, mesh=mesh, in_specs=in_specs, out_specs=out_specs, check_vma=False)
```

```python
import functools
import math

import jax
import jax.numpy as jnp
from jax import lax
from jax.experimental import pallas as pl
from jax.experimental.pallas import tpu as pltpu
from jax.sharding import PartitionSpec as P

NLON = 4096
LANES = 128
MESH = pl.DeviceIdType.MESH


def spectra_kernel(pairs, orders_ref, table_ref, coef_ref, rows_ref, send_ref, energy_ref, masked, spectra, sorted_rows, staging):
    step = pl.program_id(0)
    first_pair = lax.axis_index("blk") * pairs
    slab_rows, _, block = table_ref.shape
    packed_rows = slab_rows * pairs
    streams = masked.shape[0] // (2 * pairs)

    @pl.when(step == 0)
    def _():
        packed = coef_ref[...].reshape(packed_rows, streams)
        flipped = jnp.transpose(jnp.concatenate([packed, jnp.zeros((masked.shape[1] - packed_rows, streams), packed.dtype)], axis=0).astype(jnp.float32))
        packed_id = lax.broadcasted_iota(jnp.int32, flipped.shape, 1)
        row_id = packed_id // pairs
        pair_id = packed_id % pairs
        for pair in range(pairs):
            lower = row_id < slab_rows - 1 - orders_ref[first_pair + pair]
            mine = pair_id == pair
            for half in range(2):
                keep = mine & (lower if half == 0 else ~lower)
                start = (2 * pair + half) * streams
                masked[start : start + streams, :] = jnp.where(keep, flipped, 0.0).astype(jnp.bfloat16)

    product = jnp.dot(masked[:, :packed_rows], table_ref[...].reshape(packed_rows, block), preferred_element_type=jnp.float32)
    spectra[:, pl.ds(pl.multiple_of(step * block, block), block)] = product.astype(jnp.bfloat16)

    @pl.when(step == pl.num_programs(0) - 1)
    def _():
        lat_count = spectra.shape[1]
        fields = streams // 2
        kinds = 4 * pairs
        columns = jnp.transpose(rows_ref[...].astype(jnp.float32))
        cycle_id = lax.broadcasted_iota(jnp.int32, (LANES, lat_count), 1).astype(jnp.float32)
        total = jnp.zeros((1, kinds * fields), jnp.float32)
        half = LANES // 2
        batch = min(4, lat_count // LANES)
        for first_part in range(0, lat_count // LANES, batch):
            chosen = jnp.concatenate(
                [(columns[:, first_part + i : first_part + i + 1] == cycle_id).astype(jnp.float32).astype(jnp.bfloat16) for i in range(batch)],
                axis=0,
            )
            rows = lax.dot_general(chosen, spectra[...], (((1,), (1,)), ((), ())), preferred_element_type=jnp.float32)
            total = total + jnp.sum(rows * rows, axis=0, keepdims=True)
            for part in range(first_part, first_part + batch):
                offset = (part - first_part) * LANES
                for order in range(2 * pairs):
                    sorted_rows[part, order] = rows[offset : offset + LANES, order * streams : (order + 1) * streams]
                    even = sorted_rows[part, order, pl.ds(0, half, stride=2), :]
                    odd = sorted_rows[part, order, pl.ds(1, half, stride=2), :]
                    real = jnp.concatenate([even[:, :fields], odd[:, :fields]], axis=1)
                    imag = jnp.concatenate([even[:, fields:], odd[:, fields:]], axis=1)
                    first = part * half * kinds + 2 * order
                    staging[pl.ds(first, half, stride=kinds), :] = real
                    staging[pl.ds(first + 1, half, stride=kinds), :] = imag
        energy = jnp.zeros((1, streams), jnp.float32)
        lane_id = lax.broadcasted_iota(jnp.int32, (1, streams), 1)
        for index in range(2 * pairs):
            part = total[:, index * streams : (index + 1) * streams]
            if index % 2 == 0:
                constant = orders_ref[first_pair + index // 2] == 0
                weight = jnp.where(constant, jnp.where(lane_id < fields, 1.0, 0.0), 2.0)
            else:
                weight = 2.0
            energy = energy + weight * part
        energy_ref[...] = jnp.broadcast_to(energy, energy_ref.shape)
        send_ref[...] = staging[...].reshape(send_ref.shape).astype(jnp.bfloat16)


def exchange_kernel(n, degree, send_ref, energy_ref, orders_ref, recv_ref, basis_ref, total_ref, energies, send_sem, recv_sem, esend_sem, erecv_sem, own_sem):
    me = lax.axis_index("blk")
    barrier = pltpu.get_barrier_semaphore()

    def signal(s, carry):
        pl.semaphore_signal(barrier, inc=1, device_id={"blk": lax.rem(me + s, n)}, device_id_type=MESH)
        return carry

    lax.fori_loop(1, n, signal, 0)
    pl.semaphore_wait(barrier, n - 1)

    def block_copy(s):
        peer = lax.rem(me + s, n)
        return pltpu.make_async_remote_copy(
            src_ref=send_ref.at[peer], dst_ref=recv_ref.at[me], send_sem=send_sem.at[s], recv_sem=recv_sem.at[s],
            device_id={"blk": peer}, device_id_type=MESH)

    def energy_copy(s):
        peer = lax.rem(me + s, n)
        return pltpu.make_async_remote_copy(
            src_ref=energy_ref, dst_ref=energies.at[s], send_sem=esend_sem.at[s], recv_sem=erecv_sem.at[s],
            device_id={"blk": peer}, device_id_type=MESH)

    def start(i, carry):
        s = i + 1
        if n % 2 == 0:
            s = n // 2 + (i % 2) * ((i + 1) // 2) - (1 - i % 2) * (i // 2)
        block_copy(s).start()
        return carry

    def start_energy(s, carry):
        energy_copy(s).start()
        return carry

    lax.fori_loop(0, n - 1, start, 0)
    lax.fori_loop(1, n, start_energy, 0)
    own = pltpu.make_async_copy(send_ref.at[me], recv_ref.at[me], own_sem)
    own.start()

    rows = basis_ref.shape[0]
    row_id = lax.broadcasted_iota(jnp.int32, (rows, LANES), 0)
    lane_id = lax.broadcasted_iota(jnp.int32, (rows, LANES), 1)
    width = orders_ref.shape[1]
    pair_row = lax.broadcasted_iota(jnp.int32, (rows, width), 0) // 4
    pair_lane = lax.broadcasted_iota(jnp.int32, (rows, width), 1)
    spread = jnp.where(pair_row == pair_lane, orders_ref[...].astype(jnp.float32), 0.0)
    low = jnp.broadcast_to(jnp.sum(spread, axis=1, keepdims=True), (rows, LANES)).astype(jnp.int32)
    order = jnp.where((row_id & 2) == 0, low, degree - low)
    scale = 2.0 * math.pi / NLON
    turn = (order * (LANES * lane_id) + (row_id & 1) * (NLON // 4)) & (NLON - 1)
    fine = (order * lane_id) & (NLON - 1)
    factor = jnp.where(order == 0, 1.0, 2.0)
    coarse_angle = turn.astype(jnp.float32) * scale
    fine_angle = fine.astype(jnp.float32) * scale
    cos_coarse, sin_coarse = factor * jnp.cos(coarse_angle), factor * jnp.sin(coarse_angle)
    cos_fine, sin_fine = jnp.cos(fine_angle), jnp.sin(fine_angle)
    for tile in range(NLON // LANES):
        values = cos_coarse[:, tile : tile + 1] * cos_fine - sin_coarse[:, tile : tile + 1] * sin_fine
        basis_ref[:, tile * LANES : (tile + 1) * LANES] = values.astype(jnp.bfloat16)

    def finish_energy(s, total):
        energy_copy(s).wait()
        return total + energies[s]

    total_ref[...] = lax.fori_loop(1, n, finish_energy, energy_ref[...])

    def finish(s, carry):
        block_copy(s).wait()
        return carry

    lax.fori_loop(1, n, finish, 0)
    own.wait()


def wave_kernel(scale, recv_ref, basis_ref, total_ref, out_ref, energy_ref, held):
    groups = recv_ref.shape[1]
    depth = basis_ref.shape[0]
    fields = out_ref.shape[1]
    for group in range(groups):
        values = recv_ref[:, group, :, :].astype(jnp.float32).reshape(depth, LANES)
        held[group * LANES : (group + 1) * LANES, :] = jnp.transpose(values).astype(jnp.bfloat16)
    width = min(NLON, NLON * LANES // depth)

    @pl.loop(0, NLON // width)
    def _(tile):
        columns = pl.ds(pl.multiple_of(tile * width, width), width)
        for cycle in range(out_ref.shape[0]):
            rows = held[cycle * fields : (cycle + 1) * fields, :]
            wave = jnp.dot(rows, basis_ref[:, columns], preferred_element_type=jnp.float32)
            out_ref[cycle, :, columns] = wave.astype(jnp.bfloat16)

    energy_ref[...] = (total_ref[0:1, :fields] + total_ref[0:1, fields:]) * scale


def shards(load_coef, legendre, slab_orders, cycle_rows):
    n = lax.axis_size("blk")
    pairs, slab_rows, streams = load_coef.shape
    fields = streams // 2
    lat_count = legendre.shape[2]
    cycle_count = lat_count // n
    per_tile = LANES // fields
    groups = cycle_count // per_tile
    kinds = 4 * pairs
    degree = slab_rows - 2
    packed_rows = slab_rows * pairs
    padded = -(-packed_rows // LANES) * LANES
    table = jnp.transpose(legendre, (1, 0, 2))
    coef = jnp.transpose(load_coef, (1, 0, 2))
    steps = 4
    block = lat_count // steps
    send, energy = pl.pallas_call(
        functools.partial(spectra_kernel, pairs),
        grid_spec=pltpu.PrefetchScalarGridSpec(
            num_scalar_prefetch=1,
            grid=(steps,),
            in_specs=[
                pl.BlockSpec((slab_rows, pairs, block), lambda s, o: (0, 0, s)),
                pl.BlockSpec((slab_rows, pairs, streams), lambda s, o: (0, 0, 0), pipeline_mode=pl.Buffered(1)),
                pl.BlockSpec((lat_count // LANES, LANES), lambda s, o: (0, 0), pipeline_mode=pl.Buffered(1)),
            ],
            out_specs=[
                pl.BlockSpec((n, groups, kinds, LANES), lambda s, o: (0, 0, 0, 0)),
                pl.BlockSpec((8, streams), lambda s, o: (0, 0)),
            ],
            scratch_shapes=[
                pltpu.VMEM((2 * pairs * streams, padded), jnp.bfloat16),
                pltpu.VMEM((2 * pairs * streams, lat_count), jnp.bfloat16),
                pltpu.VMEM((lat_count // LANES, 2 * pairs, LANES, streams), jnp.float32),
                pltpu.VMEM((n * groups * kinds, LANES), jnp.float32),
            ],
        ),
        out_shape=[
            jax.ShapeDtypeStruct((n, groups, kinds, LANES), jnp.bfloat16),
            jax.ShapeDtypeStruct((8, streams), jnp.float32),
        ],
        compiler_params=pltpu.CompilerParams(dimension_semantics=("arbitrary",)),
    )(slab_orders, table, coef, cycle_rows.reshape(lat_count // LANES, LANES))
    recv, basis, total = pl.pallas_call(
        functools.partial(exchange_kernel, n, degree),
        out_shape=[
            jax.ShapeDtypeStruct((n, groups, kinds, LANES), jnp.bfloat16),
            jax.ShapeDtypeStruct((n * kinds, NLON), jnp.bfloat16),
            jax.ShapeDtypeStruct((8, streams), jnp.float32),
        ],
        in_specs=[
            pl.BlockSpec(memory_space=pl.ANY),
            pl.BlockSpec(memory_space=pltpu.VMEM),
            pl.BlockSpec(memory_space=pltpu.VMEM),
        ],
        out_specs=[
            pl.BlockSpec(memory_space=pl.ANY),
            pl.BlockSpec(memory_space=pltpu.VMEM),
            pl.BlockSpec(memory_space=pltpu.VMEM),
        ],
        scratch_shapes=[
            pltpu.VMEM((n, 8, streams), jnp.float32),
            pltpu.SemaphoreType.DMA((n,)),
            pltpu.SemaphoreType.DMA((n,)),
            pltpu.SemaphoreType.DMA((n,)),
            pltpu.SemaphoreType.DMA((n,)),
            pltpu.SemaphoreType.DMA,
        ],
        compiler_params=pltpu.CompilerParams(collective_id=0, has_side_effects=True),
    )(send, energy, slab_orders.reshape(1, n * pairs))
    step_groups = min(4, groups)
    potential, mean_square = pl.pallas_call(
        functools.partial(wave_kernel, 1.0 / lat_count),
        grid=(groups // step_groups,),
        out_shape=[
            jax.ShapeDtypeStruct((cycle_count, fields, NLON), jnp.bfloat16),
            jax.ShapeDtypeStruct((1, fields), jnp.float32),
        ],
        in_specs=[
            pl.BlockSpec((n, step_groups, kinds, LANES), lambda s: (0, s, 0, 0)),
            pl.BlockSpec((n * kinds, NLON), lambda s: (0, 0), pipeline_mode=pl.Buffered(1)),
            pl.BlockSpec((8, streams), lambda s: (0, 0), pipeline_mode=pl.Buffered(1)),
        ],
        out_specs=[
            pl.BlockSpec((step_groups * per_tile, fields, NLON), lambda s: (s, 0, 0)),
            pl.BlockSpec((1, fields), lambda s: (0, 0)),
        ],
        scratch_shapes=[pltpu.VMEM((step_groups * LANES, n * kinds), jnp.bfloat16)],
        compiler_params=pltpu.CompilerParams(dimension_semantics=("arbitrary",)),
    )(recv, basis, total)
    return potential, mean_square.reshape(fields)


def solution(mesh):
    in_specs = (P("blk", None, "rep"), P("blk", None, None), P(), P())
    out_specs = (P("blk", "rep", None), P("rep"))
    return jax.shard_map(shards, mesh=mesh, in_specs=in_specs, out_specs=out_specs, check_vma=False)
```
